512 devices in a mesh: ia: 8 (over y, core), ja: 8 (over x, z_hi), ka: 8 (over z_lo).
Axes of the slice: x: 4, y: 4, z: 16 (z_hi: 2, z_lo: 8; z = z_hi * 8 + z_lo), core: 2. Of those that a mesh axis runs over, the one named last changes fastest.
Arguments:
- block_coords: int32 [8, 8, 8, 4, 3], P('ia', 'ja', 'ka'), may hold values from 0 to 3, as said below
- live_blocks: int32 [8, 8, 8], P('ia', 'ja', 'ka'), may hold values from 1 to 4, as said below
- counts: int32 [8, 8, 8, 4, 64, 4096], P('ia', 'ja', 'ka'), may hold values from 0 to 7
- factor_a: float32 [2048, 256], P(('ia', 'ja', 'ka')), may hold values from 0.3 to 9.6
- factor_b: float32 [2048, 256], P(('ja', 'ka')), may hold values from 0.05 to 8
- factor_c: float32 [2048, 256], P('ka', 'ia'), may hold values from 0.05 to 8
Outputs:
- factor_new: float32 [2048, 256], P(('ia', 'ja', 'ka'))
The draws below stay inside these ranges and needn't reach their ends.
Inputs may be any that keep to these rules, and one draw needn't show every extreme that they name: `block_coords`: a device's slots name distinct blocks; slot 0 is always live, and every mode-1 block of the slab has a live block on some device. `live_blocks`: on some device all 4 slots are live.
All inputs are finite; a program needn't handle non-finite values.
Results may differ from the reference program's by a relative error of at most 0.00061.
Values may be sent and summed in bfloat16 or wider, within the bound.
No kernel may reach another device: no remote copies, remote signals or barrier semaphores. Data moves between devices by JAX's collectives and lax.ppermute only.
A program may use at most 64 MiB of HBM per device.

```python
import math
import jax
import jax.numpy as jnp
from jax import lax

R = 256
BS = 64
RB1 = 4
RB2 = 4
RB3 = 4
SLOTS = 4
ROWS_I = 2048
ROWS_J = 2048
ROWS_K = 2048
N_IA = 8
N_JA = 8
N_KA = 8


def draw_block_coords(key, part):
    total = N_IA * N_JA * N_KA
    many = RB1 * RB2 * RB3

    def single(index):
        sub = jax.random.fold_in(jax.random.fold_in(key, 11), index)
        first_key, other_key = jax.random.split(sub)
        group = index % (N_JA * N_KA) % RB1
        chosen = group * (RB2 * RB3) + jax.random.randint(first_key, (), 0, RB2 * RB3)
        positions = jnp.arange(many, dtype=jnp.int32)
        scores = jax.random.randint(other_key, (many,), 0, 2 ** 16) * many + positions
        scores = jnp.where(positions == chosen, 2 ** 30, scores)
        order = jnp.argsort(scores, stable=True).astype(jnp.int32)
        picked = jnp.concatenate([chosen[None].astype(jnp.int32), order[:SLOTS - 1]])
        return jnp.stack([picked // (RB2 * RB3), picked // RB3 % RB2, picked % RB3], axis=-1)
    result = jax.vmap(single)(jnp.arange(total, dtype=jnp.int32))
    return result.reshape(N_IA, N_JA, N_KA, SLOTS, 3).astype(jnp.int32)


def draw_live_blocks(key, part):
    total = N_IA * N_JA * N_KA
    key_base, key_busy, key_forced = jax.random.split(jax.random.fold_in(key, 23), 3)
    base = jax.random.randint(key_base, (total,), 1, max(2, SLOTS // 2 + 1))
    busy = jax.random.randint(key_busy, (total,), 0, 8) == 0
    forced = jax.random.randint(key_forced, (), 0, total)
    result = jnp.where(busy | (jnp.arange(total) == forced), SLOTS, base)
    return result.reshape(N_IA, N_JA, N_KA).astype(jnp.int32)


def topic_factor(key, seed_offset, row_count, lowest, highest, factor_boost):
    folded = jax.random.fold_in(key, seed_offset)
    key_level, key_marked = jax.random.split(folded)
    base_level = jnp.exp(jax.random.uniform(key_level, (row_count, R), jnp.float32, math.log(lowest), math.log(highest)))
    marked = jax.random.randint(key_marked, (row_count, R), 0, 32) == 0
    return jnp.where(marked, base_level * factor_boost, base_level).astype(jnp.float32)


def draw_factor_a(key, part):
    return topic_factor(key, 31, ROWS_I, 0.3, 1.2, 8.0)


def draw_factor_b(key, part):
    factor_boost = 30.0
    return topic_factor(key, 37, ROWS_J, 0.05, 0.2, factor_boost)


def draw_factor_c(key, part):
    factor_boost = 30.0
    return topic_factor(key, 41, ROWS_K, 0.05, 0.2, factor_boost)


def plant(values, own_key, low, top_value):
    index_at = [jax.random.randint(jax.random.fold_in(own_key, axis), (), 0, length) for axis, length in enumerate(values.shape)]
    widest = values.shape.index(max(values.shape))
    neighbour = index_at[:widest] + [(index_at[widest] + 1) % values.shape[widest]] + index_at[widest + 1:]
    return values.at[tuple(index_at)].set(low).at[tuple(neighbour)].set(top_value)


def setup_inputs(seed: int = 0) -> dict:
    streams_of = jax.random.split(jax.random.key(seed), 7)
    return {
        "block_coords": draw_block_coords(jax.random.fold_in(streams_of[6], 71), 0),
        "live_blocks": draw_live_blocks(jax.random.fold_in(streams_of[6], 71), 0),
        "counts": plant(jax.random.randint(streams_of[2], (N_IA, N_JA, N_KA, SLOTS, BS, BS * BS), 0, 8), jax.random.fold_in(streams_of[2], 1), 0, 7).astype(jnp.int32),
        "factor_a": draw_factor_a(jax.random.fold_in(streams_of[6], 71), 0),
        "factor_b": draw_factor_b(jax.random.fold_in(streams_of[6], 71), 0),
        "factor_c": draw_factor_c(jax.random.fold_in(streams_of[6], 71), 0),
    }


def reference(block_coords, live_blocks, counts, factor_a, factor_b, factor_c):
    devices_all = N_IA * N_JA * N_KA
    total = devices_all * SLOTS
    flat_coords = block_coords.reshape(total, 3)
    entry = jnp.arange(total, dtype=jnp.int32)
    device = entry // SLOTS
    slot = entry % SLOTS
    a_index = device // (N_JA * N_KA)
    b_index = (device // N_KA) % N_JA
    c_index = device % N_KA
    weight = (slot < live_blocks.reshape(devices_all)[device]).astype(jnp.float32)
    block_i = (a_index * RB1 + flat_coords[:, 0]).astype(jnp.int32)
    block_j = (b_index * RB2 + flat_coords[:, 1]).astype(jnp.int32)
    block_k = (c_index * RB3 + flat_coords[:, 2]).astype(jnp.int32)
    flat_counts = counts.reshape(total, BS, BS * BS)
    sums_b = factor_b.reshape(N_JA * RB2, BS, R).sum(axis=1)
    sums_c = factor_c.reshape(N_KA * RB3, BS, R).sum(axis=1)
    masses = sums_b[block_j] * sums_c[block_k] * weight[:, None]
    mass = jax.ops.segment_sum(masses, block_i, num_segments=N_IA * RB1)
    mass_rows = jnp.repeat(mass, BS, axis=0)

    def accumulate(factor):
        factor_low = factor.astype(jnp.bfloat16)

        def step(phi, item):
            gi, gj, gk, w, block_counts = item
            rows_b = lax.dynamic_slice_in_dim(factor_b, gj * BS, BS, 0)
            rows_c = lax.dynamic_slice_in_dim(factor_c, gk * BS, BS, 0)
            panel = (rows_b[:, None, :] * rows_c[None, :, :]).reshape(BS * BS, R).astype(jnp.bfloat16)
            block_a = lax.dynamic_slice_in_dim(factor_low, gi * BS, BS, 0)
            model = lax.dot_general(block_a, panel, (((1,), (1,)), ((), ())), preferred_element_type=jnp.float32)
            ratio = (block_counts.astype(jnp.float32) / model).astype(jnp.bfloat16)
            part = jnp.dot(ratio, panel, preferred_element_type=jnp.float32) * w
            old = lax.dynamic_slice_in_dim(phi, gi * BS, BS, 0)
            return lax.dynamic_update_slice_in_dim(phi, old + part, gi * BS, 0), None

        start = jnp.zeros((N_IA * RB1 * BS, R), jnp.float32)
        phi, _ = lax.scan(step, start, (block_i, block_j, block_k, weight, flat_counts))
        return phi

    first = factor_a * accumulate(factor_a) / mass_rows
    return first * accumulate(first) / mass_rows
```

```python
import jax
import jax.numpy as jnp
from jax import lax
from jax.experimental import pallas as pl
from jax.experimental.pallas import tpu as pltpu
from jax.sharding import Mesh, PartitionSpec as P

R = 256
BS = 64
RB1 = 4
SLOTS = 4
SPAN = 1024
F32 = jnp.float32
BF16 = jnp.bfloat16

IA = "ia"
JX = "jx"
JZ = "jz"
KA = "ka"
JK = (JX, JZ, KA)
ZK = (JZ, KA)


def swap(x, axis):
    return lax.all_to_all(x, axis, split_axis=0, concat_axis=0, tiled=True)


def from_everyone(x, axis):
    return swap(jnp.broadcast_to(x, (lax.axis_size(axis), *x.shape)), axis)


def aligned(start, size):
    return pl.ds(pl.multiple_of(start * size, size), size)


def block_order(eighth, half):
    return half * 8 + eighth


def prep_kernel(coords, live, both, rows_c, mass):
    rows_c[...] = jnp.swapaxes(both[:, 32:, :].reshape(R, R), 0, 1)
    mass[...] = jnp.zeros_like(mass)
    for slot in range(SLOTS):

        @pl.when(slot < live[0])
        def _():
            g = coords[slot * 3]
            j = coords[slot * 3 + 1]
            k = coords[slot * 3 + 2]
            piece_b = both[:, aligned(j, 8), :].reshape(BS, R)
            piece_c = rows_c[aligned(k, BS), :]
            sum_b = jnp.sum(piece_b, axis=0, keepdims=True)
            sum_c = jnp.sum(piece_c, axis=0, keepdims=True)
            mass[g, 0:1, :] = mass[g, 0:1, :] + sum_b * sum_c


def prepare(coords, live, both):
    return pl.pallas_call(
        prep_kernel,
        grid_spec=pltpu.PrefetchScalarGridSpec(
            num_scalar_prefetch=2,
            grid=(1,),
            in_specs=[pl.BlockSpec((8, 64, R), lambda s, *_: (0, 0, 0))],
            out_specs=[
                pl.BlockSpec((R, R), lambda s, *_: (0, 0)),
                pl.BlockSpec((RB1, 8, R), lambda s, *_: (0, 0, 0)),
            ],
        ),
        out_shape=[
            jax.ShapeDtypeStruct((R, R), F32),
            jax.ShapeDtypeStruct((RB1, 8, R), F32),
        ],
        name="prepare",
    )(coords, live, both)


def pass_kernel(with_mass):
    def kernel(coords, live, counts, factor, both, rows_c, *rest):
        if with_mass:
            mass, out, panel = rest
        else:
            out, panel = rest
        slot = pl.program_id(0)

        @pl.when(slot == 0)
        def _():
            out[:, :BS, :] = jnp.zeros((RB1, BS, R), F32)
            if with_mass:
                out[:, BS:, :] = mass[...]

        @pl.when(slot < live[0])
        def _():
            i = coords[slot * 3]
            j = coords[slot * 3 + 1]
            k = coords[slot * 3 + 2]
            piece_a = factor[aligned(i, BS), :]
            piece_c = rows_c[aligned(k, BS), :]
            for half in range(2):
                for eighth in range(8):
                    rows_b = both[eighth, aligned(j, 8), :]
                    first = block_order(eighth, half) * 4
                    for q in range(4):
                        row = rows_b[half * 4 + q : half * 4 + q + 1, :]
                        panel[(first + q) * BS : (first + q + 1) * BS, :] = (
                            row * piece_c
                        ).astype(BF16)
            total = jnp.zeros((BS, R), F32)
            for start in range(0, BS * BS, SPAN):
                piece = panel[start : start + SPAN, :]
                model = lax.dot_general(
                    piece_a, piece, (((1,), (1,)), ((), ())), preferred_element_type=F32
                )
                hits = counts[0, :, start : start + SPAN].astype(F32)
                ratio = (hits / model).astype(BF16)
                total = total + jnp.dot(ratio, piece, preferred_element_type=F32)
            out[i, :BS, :] = out[i, :BS, :] + total

    return kernel


def run_pass(coords, live, counts, factor, both, rows_c, mass=None):
    rows = BS if mass is None else BS + 8
    in_specs = [
        pl.BlockSpec((1, BS, BS * BS), lambda s, *_: (s, 0, 0)),
        pl.BlockSpec((R, R), lambda s, *_: (0, 0)),
        pl.BlockSpec((8, 64, R), lambda s, *_: (0, 0, 0)),
        pl.BlockSpec((R, R), lambda s, *_: (0, 0)),
    ]
    args = [counts, factor, both, rows_c]
    if mass is not None:
        in_specs.append(pl.BlockSpec((RB1, 8, R), lambda s, *_: (0, 0, 0)))
        args.append(mass)
    return pl.pallas_call(
        pass_kernel(mass is not None),
        grid_spec=pltpu.PrefetchScalarGridSpec(
            num_scalar_prefetch=2,
            grid=(SLOTS,),
            in_specs=in_specs,
            out_specs=pl.BlockSpec((RB1, rows, R), lambda s, *_: (0, 0, 0)),
            scratch_shapes=[pltpu.VMEM((BS * BS, R), BF16)],
        ),
        out_shape=jax.ShapeDtypeStruct((RB1, rows, R), F32),
        compiler_params=pltpu.CompilerParams(dimension_semantics=("arbitrary",)),
        name="one_pass",
    )(coords, live, *args)


def local(block_coords, live_blocks, counts, factor_a, factor_b, factor_c):
    coords = block_coords.reshape(SLOTS * 3)
    live = live_blocks.reshape(1)
    hits = counts.reshape(SLOTS, BS, BS * BS)
    mine_b = lax.dynamic_slice_in_dim(factor_b, lax.axis_index(IA) * 4, 4, 0)
    share_b = from_everyone(mine_b, KA).reshape(32, R)
    both = from_everyone(jnp.concatenate([share_b, factor_c.T], axis=0), IA)
    low = from_everyone(factor_a.astype(BF16), JK).reshape(R, R)
    rows_c, mass = prepare(coords, live, both)

    phi = run_pass(coords, live, hits, low, both, rows_c, mass)
    part = swap(phi, JX).sum(axis=0)
    rows = jnp.concatenate(
        [part[:BS].reshape(16, 4, R), jnp.broadcast_to(part[BS:, :][None, :4], (16, 4, R))], axis=1
    )
    mine = swap(rows, ZK).sum(axis=0)
    my_mass = mine[4:5]
    first = factor_a * mine[:4] / my_mass
    low = from_everyone(first.astype(BF16), JK).reshape(R, R)
    phi = run_pass(coords, live, hits, low, both, rows_c)
    part = swap(phi, JX).sum(axis=0)
    mine = swap(part.reshape(16, 4, R), ZK).sum(axis=0)
    return first * mine / my_mass


def solution(mesh):
    shape = mesh.shape
    fine = Mesh(
        mesh.devices.reshape(shape["ia"], shape["ja"] // 2, 2, shape["ka"]), (IA, JX, JZ, KA)
    )
    placed = (
        P(IA, (JX, JZ), KA, None, None),
        P(IA, (JX, JZ), KA),
        P(IA, (JX, JZ), KA, None, None, None),
        P((IA, JX, JZ, KA), None),
        P((JX, JZ, KA), None),
        P(KA, IA),
    )
    return jax.shard_map(
        local, mesh=fine, in_specs=placed, out_specs=P((IA, JX, JZ, KA), None), check_vma=False
    )
```

```python
import jax
import jax.numpy as jnp
from jax import lax
from jax.experimental import pallas as pl
from jax.experimental.pallas import tpu as pltpu
from jax.sharding import Mesh, PartitionSpec as P


R = 256
BS = 64
RB1 = 4
SLOTS = 4
SPAN = 1024
F32 = jnp.float32
F16 = jnp.float16
PHI_SCALE = 0.25
MASS_SCALE = 1.0 / 32.0
BF16 = jnp.bfloat16

IA = "ia"
JX = "jx"
JZ = "jz"
KA = "ka"
JK = (JX, JZ, KA)
ZK = (JZ, KA)


def swap(x, axis):
    return lax.all_to_all(x, axis, split_axis=0, concat_axis=0, tiled=True)


def from_everyone(x, axis):
    return swap(jnp.broadcast_to(x, (lax.axis_size(axis), *x.shape)), axis)


def aligned(start, size):
    return pl.ds(pl.multiple_of(start * size, size), size)


def block_order(eighth, half):
    return half * 8 + eighth


def prep_kernel(coords, live, both, rows_c, mass):
    rows_c[...] = jnp.swapaxes(both[:, 32:, :].reshape(R, R), 0, 1)
    mass[...] = jnp.zeros_like(mass)
    for slot in range(SLOTS):

        @pl.when(slot < live[0])
        def _():
            g = coords[slot * 3]
            j = coords[slot * 3 + 1]
            k = coords[slot * 3 + 2]
            piece_b = both[:, aligned(j, 8), :].reshape(BS, R)
            piece_c = rows_c[aligned(k, BS), :]
            sum_b = jnp.sum(piece_b, axis=0, keepdims=True)
            sum_c = jnp.sum(piece_c, axis=0, keepdims=True)
            mass[g, 0:1, :] = mass[g, 0:1, :] + sum_b * sum_c


def prepare(coords, live, both):
    whole = pl.BlockSpec(memory_space=pltpu.VMEM)
    scalars = pl.BlockSpec(memory_space=pltpu.SMEM)
    return pl.pallas_call(
        prep_kernel,
        in_specs=[scalars, scalars, whole],
        out_specs=[whole, whole],
        out_shape=[
            jax.ShapeDtypeStruct((R, R), F32),
            jax.ShapeDtypeStruct((RB1, 8, R), F32),
        ],
        compiler_params=pltpu.CompilerParams(vmem_limit_bytes=8 << 20),
        name="prepare",
    )(coords, live, both)


def pass_kernel(coords, live, counts, factor, both, rows_c, out, panel, hits, arrived):
    def fetch(slot):
        return pltpu.make_async_copy(counts.at[slot], hits.at[slot], arrived.at[slot])

    for slot in range(SLOTS):

        @pl.when(slot < live[0])
        def _():
            fetch(slot).start()

    out[...] = jnp.zeros_like(out)

    def step(slot, carry):
        i = coords[slot * 3]
        j = coords[slot * 3 + 1]
        k = coords[slot * 3 + 2]
        piece_a = factor[aligned(i, BS), :]
        piece_c = rows_c[aligned(k, BS), :]
        for half in range(2):
            for eighth in range(8):
                rows_b = both[eighth, aligned(j, 8), :]
                first = block_order(eighth, half) * 4
                for q in range(4):
                    row = rows_b[half * 4 + q : half * 4 + q + 1, :]
                    panel[(first + q) * BS : (first + q + 1) * BS, :] = (
                        row * piece_c
                    ).astype(BF16)
        fetch(slot).wait()
        total = jnp.zeros((BS, R), F32)
        for start in range(0, BS * BS, SPAN):
            piece = panel[start : start + SPAN, :]
            model = lax.dot_general(
                piece_a, piece, (((1,), (1,)), ((), ())), preferred_element_type=F32
            )
            count = hits[slot, :, start : start + SPAN].astype(F32)
            ratio = (count / model).astype(BF16)
            total = total + jnp.dot(ratio, piece, preferred_element_type=F32)
        out[i] = out[i] + total * (piece_a.astype(F32) * PHI_SCALE)
        return carry

    lax.fori_loop(0, live[0], step, 0)


def run_pass(coords, live, counts, factor, both, rows_c):
    whole = pl.BlockSpec(memory_space=pltpu.VMEM)
    scalars = pl.BlockSpec(memory_space=pltpu.SMEM)
    return pl.pallas_call(
        pass_kernel,
        in_specs=[scalars, scalars, pl.BlockSpec(memory_space=pltpu.HBM), whole, whole, whole],
        out_specs=whole,
        scratch_shapes=[
            pltpu.VMEM((BS * BS, R), BF16),
            pltpu.VMEM((SLOTS, BS, BS * BS), jnp.int32),
            pltpu.SemaphoreType.DMA((SLOTS,)),
        ],
        out_shape=jax.ShapeDtypeStruct((RB1, BS, R), F32),
        compiler_params=pltpu.CompilerParams(vmem_limit_bytes=24 << 20),
        name="one_pass",
    )(coords, live, pltpu.with_memory_space_constraint(counts, pltpu.HBM), factor, both, rows_c)


def rounded(x):
    return lax.reduce_precision(x, exponent_bits=8, mantissa_bits=7)


def unweighted(factor, low):
    return jnp.where(low == 0.0, 0.0, factor / jnp.where(low == 0.0, 1.0, low))


def local(block_coords, live_blocks, counts, factor_a, factor_b, factor_c):
    coords = block_coords.reshape(SLOTS * 3)
    live = live_blocks.reshape(1)
    hits = counts.reshape(SLOTS, BS, BS * BS)
    low_a = rounded(factor_a)
    mine_b = lax.dynamic_slice_in_dim(factor_b, lax.axis_index(IA) * 4, 4, 0)
    column = from_everyone(jnp.concatenate([low_a.astype(F16), mine_b.astype(F16)], axis=0), ZK)
    share_b = lax.dynamic_slice_in_dim(column[:, 4:], lax.axis_index(JZ) * 8, 8, 0)
    both = from_everyone(
        jnp.concatenate([share_b.reshape(32, R), factor_c.T.astype(F16)], axis=0), IA
    ).astype(F32)
    low = from_everyone(column[:, :4].reshape(64, R).astype(BF16), JX).reshape(R, R)
    rows_c, mass = prepare(coords, live, both)

    phi = run_pass(coords, live, hits, low, both, rows_c)
    mass_rows = jnp.broadcast_to(
        (mass[:, 0, :] * MASS_SCALE).astype(F16).reshape(RB1, 1, 2, 128), (RB1, 16, 2, 128)
    ).reshape(64, 2, 128)
    sent = jnp.concatenate([phi.astype(F16).reshape(64, 2, 512), mass_rows], axis=2)
    got = swap(sent, JK).astype(F32).sum(axis=0)
    scale = (MASS_SCALE / PHI_SCALE) / got[:, 512:].reshape(1, R)
    first = unweighted(factor_a, low_a) * got[:, :512].reshape(4, R) * scale
    low_first = rounded(first)
    low = from_everyone(low_first.astype(BF16), JK).reshape(R, R)
    phi = run_pass(coords, live, hits, low, both, rows_c)
    mine = swap(phi.astype(F16).reshape(64, 4, R), JK).astype(F32).sum(axis=0)
    return unweighted(first, low_first) * mine * scale


def solution(mesh):
    shape = mesh.shape
    fine = Mesh(
        mesh.devices.reshape(shape["ia"], shape["ja"] // 2, 2, shape["ka"]), (IA, JX, JZ, KA)
    )
    placed = (
        P(IA, (JX, JZ), KA, None, None),
        P(IA, (JX, JZ), KA),
        P(IA, (JX, JZ), KA, None, None, None),
        P((IA, JX, JZ, KA), None),
        P((JX, JZ, KA), None),
        P(KA, IA),
    )
    return jax.shard_map(
        local, mesh=fine, in_specs=placed, out_specs=P((IA, JX, JZ, KA), None), check_vma=False
    )
```

```python
import jax
import jax.numpy as jnp
from jax import lax
from jax.experimental import pallas as pl
from jax.experimental.pallas import tpu as pltpu
from jax.sharding import Mesh, PartitionSpec as P


R = 256
BS = 64
RB1 = 4
SLOTS = 4
SPAN = 1024
F32 = jnp.float32
F16 = jnp.float16
PHI_SCALE = 0.25
MASS_SCALE = 1.0 / 32.0
BF16 = jnp.bfloat16

IA = "ia"
JX = "jx"
JZ = "jz"
KA = "ka"
JK = (JX, JZ, KA)
ZK = (JZ, KA)


def swap(x, axis):
    return lax.all_to_all(x, axis, split_axis=0, concat_axis=0, tiled=True)


def from_everyone(x, axis):
    return swap(jnp.broadcast_to(x, (lax.axis_size(axis), *x.shape)), axis)


def aligned(start, size):
    return pl.ds(pl.multiple_of(start * size, size), size)


def whole():
    return pl.BlockSpec(memory_space=pltpu.VMEM)


def scalars():
    return pl.BlockSpec(memory_space=pltpu.SMEM)


def load_kernel(live, counts, hits, raw, arrived):
    def fetch(slot):
        return pltpu.make_async_copy(counts.at[slot], raw.at[slot], arrived.at[slot])

    for slot in range(SLOTS):

        @pl.when(slot < live[0])
        def _():
            fetch(slot).start()

    def step(slot, carry):
        fetch(slot).wait()
        hits[slot] = raw[slot].astype(F32).astype(BF16)
        return carry

    lax.fori_loop(0, live[0], step, 0)


def load(live, counts):
    return pl.pallas_call(
        load_kernel,
        in_specs=[scalars(), pl.BlockSpec(memory_space=pltpu.HBM)],
        out_specs=whole(),
        out_shape=jax.ShapeDtypeStruct((SLOTS, BS, BS * BS), BF16),
        scratch_shapes=[
            pltpu.VMEM((SLOTS, BS, BS * BS), jnp.int32),
            pltpu.SemaphoreType.DMA((SLOTS,)),
        ],
        compiler_params=pltpu.CompilerParams(vmem_limit_bytes=10 << 20),
        name="load",
    )(live, pltpu.with_memory_space_constraint(counts, pltpu.HBM))


def block_order(eighth, half):
    return half * 8 + eighth


def prep_kernel(coords, live, both, rows_c, mass):
    rows_c[...] = jnp.swapaxes(both[:, 32:, :].reshape(R, R), 0, 1)
    mass[...] = jnp.zeros_like(mass)
    for slot in range(SLOTS):

        @pl.when(slot < live[0])
        def _():
            g = coords[slot * 3]
            j = coords[slot * 3 + 1]
            k = coords[slot * 3 + 2]
            piece_b = both[:, aligned(j, 8), :].reshape(BS, R)
            piece_c = rows_c[aligned(k, BS), :]
            sum_b = jnp.sum(piece_b, axis=0, keepdims=True)
            sum_c = jnp.sum(piece_c, axis=0, keepdims=True)
            mass[g, 0:1, :] = mass[g, 0:1, :] + sum_b * sum_c


def prepare(coords, live, both):
    return pl.pallas_call(
        prep_kernel,
        in_specs=[scalars(), scalars(), whole()],
        out_specs=[whole(), whole()],
        out_shape=[
            jax.ShapeDtypeStruct((R, R), F32),
            jax.ShapeDtypeStruct((RB1, 8, R), F32),
        ],
        compiler_params=pltpu.CompilerParams(vmem_limit_bytes=8 << 20),
        name="prepare",
    )(coords, live, both)


def pass_kernel(coords, live, hits, factor, both, rows_c, out, panel):
    out[...] = jnp.zeros_like(out)

    def step(slot, carry):
        i = coords[slot * 3]
        j = coords[slot * 3 + 1]
        k = coords[slot * 3 + 2]
        piece_a = factor[aligned(i, BS), :]
        piece_c = rows_c[aligned(k, BS), :]
        for half in range(2):
            for eighth in range(8):
                rows_b = both[eighth, aligned(j, 8), :]
                first = block_order(eighth, half) * 4
                for q in range(4):
                    row = rows_b[half * 4 + q : half * 4 + q + 1, :]
                    panel[(first + q) * BS : (first + q + 1) * BS, :] = (
                        row * piece_c
                    ).astype(BF16)
        total = jnp.zeros((BS, R), F32)
        for start in range(0, BS * BS, SPAN):
            piece = panel[start : start + SPAN, :]
            model = lax.dot_general(
                piece_a, piece, (((1,), (1,)), ((), ())), preferred_element_type=F32
            )
            count = hits[slot, :, start : start + SPAN].astype(F32)
            ratio = (count / model).astype(BF16)
            total = total + jnp.dot(ratio, piece, preferred_element_type=F32)
        out[i] = out[i] + total * (piece_a.astype(F32) * PHI_SCALE)
        return carry

    lax.fori_loop(0, live[0], step, 0)


def run_pass(coords, live, hits, factor, both, rows_c):
    return pl.pallas_call(
        pass_kernel,
        in_specs=[scalars(), scalars()] + [whole()] * 4,
        out_specs=whole(),
        scratch_shapes=[pltpu.VMEM((BS * BS, R), BF16)],
        out_shape=jax.ShapeDtypeStruct((RB1, BS, R), F32),
        compiler_params=pltpu.CompilerParams(vmem_limit_bytes=16 << 20),
        name="one_pass",
    )(coords, live, hits, factor, both, rows_c)


def rounded(x):
    return lax.reduce_precision(x, exponent_bits=8, mantissa_bits=7)


def unweighted(factor, low):
    return jnp.where(low == 0.0, 0.0, factor / jnp.where(low == 0.0, 1.0, low))


def local(block_coords, live_blocks, counts, factor_a, factor_b, factor_c):
    coords = block_coords.reshape(SLOTS * 3)
    live = live_blocks.reshape(1)
    low_a = rounded(factor_a)
    mine_b = lax.dynamic_slice_in_dim(factor_b, lax.axis_index(IA) * 4, 4, 0)
    column = from_everyone(jnp.concatenate([low_a.astype(F16), mine_b.astype(F16)], axis=0), ZK)
    hits = load(live, counts.reshape(SLOTS, BS, BS * BS))
    share_b = lax.dynamic_slice_in_dim(column[:, 4:], lax.axis_index(JZ) * 8, 8, 0)
    both = from_everyone(
        jnp.concatenate([share_b.reshape(32, R), factor_c.T.astype(F16)], axis=0), IA
    ).astype(F32)
    low = from_everyone(column[:, :4].reshape(64, R).astype(BF16), JX).reshape(R, R)
    rows_c, mass = prepare(coords, live, both)

    phi = run_pass(coords, live, hits, low, both, rows_c)
    mass_rows = jnp.broadcast_to(
        (mass[:, 0, :] * MASS_SCALE).astype(F16).reshape(RB1, 1, 2, 128), (RB1, 16, 2, 128)
    ).reshape(64, 2, 128)
    sent = jnp.concatenate([phi.astype(F16).reshape(64, 2, 512), mass_rows], axis=2)
    got = swap(sent, JK).astype(F32).sum(axis=0)
    scale = (MASS_SCALE / PHI_SCALE) / got[:, 512:].reshape(1, R)
    first = unweighted(factor_a, low_a) * got[:, :512].reshape(4, R) * scale
    low_first = rounded(first)
    low = from_everyone(low_first.astype(BF16), JK).reshape(R, R)
    phi = run_pass(coords, live, hits, low, both, rows_c)
    mine = swap(phi.astype(F16).reshape(64, 4, R), JK).astype(F32).sum(axis=0)
    return unweighted(first, low_first) * mine * scale


def solution(mesh):
    shape = mesh.shape
    fine = Mesh(
        mesh.devices.reshape(shape["ia"], shape["ja"] // 2, 2, shape["ka"]), (IA, JX, JZ, KA)
    )
    placed = (
        P(IA, (JX, JZ), KA, None, None),
        P(IA, (JX, JZ), KA),
        P(IA, (JX, JZ), KA, None, None, None),
        P((IA, JX, JZ, KA), None),
        P((JX, JZ, KA), None),
        P(KA, IA),
    )
    return jax.shard_map(
        local, mesh=fine, in_specs=placed, out_specs=P((IA, JX, JZ, KA), None), check_vma=False
    )
```

```python
import functools

import jax
import jax.numpy as jnp
from jax import lax
from jax.experimental import pallas as pl
from jax.experimental.pallas import tpu as pltpu
from jax.sharding import Mesh, PartitionSpec as P


R = 256
BS = 64
RB1 = 4
SLOTS = 4
SPAN = 1024
F32 = jnp.float32
F16 = jnp.float16
PHI_SCALE = 0.25
MASS_SCALE = 1.0 / 32.0
BF16 = jnp.bfloat16


IA = "ia"
JX = "jx"
JZ = "jz"
KA = "ka"
JK = (JX, JZ, KA)
ZK = (JZ, KA)


def swap(x, axis):
    return lax.all_to_all(x, axis, split_axis=0, concat_axis=0, tiled=True)


def from_everyone(x, axis):
    return swap(jnp.broadcast_to(x, (lax.axis_size(axis), *x.shape)), axis)


def aligned(start, size):
    return pl.ds(pl.multiple_of(start * size, size), size)


def whole():
    return pl.BlockSpec(memory_space=pltpu.VMEM)


def scalars():
    return pl.BlockSpec(memory_space=pltpu.SMEM)


def load_kernel(live, counts, hits, raw, arrived):
    def fetch(slot):
        return pltpu.make_async_copy(counts.at[slot], raw.at[slot], arrived.at[slot])

    for slot in range(SLOTS):

        @pl.when(slot < live[0])
        def _():
            fetch(slot).start()

    def step(slot, carry):
        fetch(slot).wait()
        hits[slot] = raw[slot].astype(F32).astype(BF16)
        return carry

    lax.fori_loop(0, live[0], step, 0)


def load(live, counts):
    return pl.pallas_call(
        load_kernel,
        in_specs=[scalars(), pl.BlockSpec(memory_space=pltpu.HBM)],
        out_specs=whole(),
        out_shape=jax.ShapeDtypeStruct((SLOTS, BS, BS * BS), BF16),
        scratch_shapes=[
            pltpu.VMEM((SLOTS, BS, BS * BS), jnp.int32),
            pltpu.SemaphoreType.DMA((SLOTS,)),
        ],
        compiler_params=pltpu.CompilerParams(vmem_limit_bytes=10 << 20),
        name="load",
    )(live, pltpu.with_memory_space_constraint(counts, pltpu.HBM))


def block_order(eighth, half):
    return half * 8 + eighth


def prep_kernel(coords, live, both, rows_c, mass):
    rows_c[...] = jnp.swapaxes(both[:, 32:, :].reshape(R, R), 0, 1)
    mass[...] = jnp.zeros_like(mass)
    for slot in range(SLOTS):

        @pl.when(slot < live[0])
        def _():
            g = coords[slot * 3]
            j = coords[slot * 3 + 1]
            k = coords[slot * 3 + 2]
            piece_b = both[:, aligned(j, 8), :].reshape(BS, R)
            piece_c = rows_c[aligned(k, BS), :]
            sum_b = jnp.sum(piece_b, axis=0, keepdims=True)
            sum_c = jnp.sum(piece_c, axis=0, keepdims=True)
            mass[g, 0:1, :] = mass[g, 0:1, :] + sum_b * sum_c


def prepare(coords, live, both):
    return pl.pallas_call(
        prep_kernel,
        in_specs=[scalars(), scalars(), whole()],
        out_specs=[whole(), whole()],
        out_shape=[
            jax.ShapeDtypeStruct((R, R), F32),
            jax.ShapeDtypeStruct((RB1, 8, R), F32),
        ],
        compiler_params=pltpu.CompilerParams(vmem_limit_bytes=8 << 20),
        name="prepare",
    )(coords, live, both)


def pass_kernel(pieces, coords, live, hits, both, rows_c, *rest):
    if pieces:
        place, *parts, out, panel, factor = rest
        for back in range(RB1):
            factor[back * BS : (back + 1) * BS, :] = parts[back][...]
    else:
        factor, out, panel = rest
    out[...] = jnp.zeros_like(out)

    def step(slot, carry):
        i = coords[slot * 3]
        j = coords[slot * 3 + 1]
        k = coords[slot * 3 + 2]
        piece_a = factor[aligned((place[0] - i) & (RB1 - 1) if pieces else i, BS), :]
        piece_c = rows_c[aligned(k, BS), :]
        for half in range(2):
            for eighth in range(8):
                rows_b = both[eighth, aligned(j, 8), :]
                first = block_order(eighth, half) * 4
                for q in range(4):
                    row = rows_b[half * 4 + q : half * 4 + q + 1, :]
                    panel[(first + q) * BS : (first + q + 1) * BS, :] = (
                        row * piece_c
                    ).astype(BF16)
        total = jnp.zeros((BS, R), F32)
        for start in range(0, BS * BS, SPAN):
            piece = panel[start : start + SPAN, :]
            model = lax.dot_general(
                piece_a, piece, (((1,), (1,)), ((), ())), preferred_element_type=F32
            )
            count = hits[slot, :, start : start + SPAN].astype(F32)
            ratio = (count / model).astype(BF16)
            total = total + jnp.dot(ratio, piece, preferred_element_type=F32)
        out[i] = out[i] + total * (piece_a.astype(F32) * PHI_SCALE)
        return carry

    lax.fori_loop(0, live[0], step, 0)


def run_pass(coords, live, hits, both, rows_c, place, *factor):
    pieces = place is not None
    scratch = [pltpu.VMEM((BS * BS, R), BF16)]
    if pieces:
        scratch.append(pltpu.VMEM((R, R), BF16))
    return pl.pallas_call(
        functools.partial(pass_kernel, pieces),
        in_specs=[scalars(), scalars(), whole(), whole(), whole()]
        + ([scalars()] if pieces else [])
        + [whole()] * len(factor),
        out_specs=whole(),
        scratch_shapes=scratch,
        out_shape=jax.ShapeDtypeStruct((RB1, BS, R), F32),
        compiler_params=pltpu.CompilerParams(vmem_limit_bytes=16 << 20),
        name="one_pass",
    )(coords, live, hits, both, rows_c, *([place] if pieces else []), *factor)


def rounded(x):
    return lax.reduce_precision(x, exponent_bits=8, mantissa_bits=7)


def unweighted(factor, low):
    return jnp.where(low == 0.0, 0.0, factor / jnp.where(low == 0.0, 1.0, low))


def local(block_coords, live_blocks, counts, factor_a, factor_b, factor_c):
    coords = block_coords.reshape(SLOTS * 3)
    live = live_blocks.reshape(1)
    low_a = rounded(factor_a)
    mine_b = lax.dynamic_slice_in_dim(factor_b, lax.axis_index(IA) * 4, 4, 0)
    column = from_everyone(jnp.concatenate([low_a.astype(F16), mine_b.astype(F16)], axis=0), ZK)
    hits = load(live, counts.reshape(SLOTS, BS, BS * BS))
    share_b = lax.dynamic_slice_in_dim(column[:, 4:], lax.axis_index(JZ) * 8, 8, 0)
    both = from_everyone(
        jnp.concatenate([share_b.reshape(32, R), factor_c.T.astype(F16)], axis=0), IA
    ).astype(F32)
    own = column[:, :4].reshape(BS, R).astype(BF16)
    many = lax.axis_size(JX)
    pieces = [own] + [
        lax.ppermute(own, JX, [(x, (x + back) % many) for x in range(many)])
        for back in range(1, many)
    ]
    rows_c, mass = prepare(coords, live, both)

    place = lax.axis_index(JX).reshape(1)
    phi = run_pass(coords, live, hits, both, rows_c, place, *pieces)
    mass_rows = jnp.broadcast_to(
        (mass[:, 0, :] * MASS_SCALE).astype(F16).reshape(RB1, 1, 2, 128), (RB1, 16, 2, 128)
    ).reshape(64, 2, 128)
    sent = jnp.concatenate([phi.astype(F16).reshape(64, 2, 512), mass_rows], axis=2)
    got = swap(sent, JK).astype(F32).sum(axis=0)
    scale = (MASS_SCALE / PHI_SCALE) / got[:, 512:].reshape(1, R)
    first = unweighted(factor_a, low_a) * got[:, :512].reshape(4, R) * scale
    low_first = rounded(first)
    low = from_everyone(low_first.astype(BF16), JK).reshape(R, R)
    phi = run_pass(coords, live, hits, both, rows_c, None, low)
    mine = swap(phi.astype(F16).reshape(64, 4, R), JK).astype(F32).sum(axis=0)
    return unweighted(first, low_first) * mine * scale


def solution(mesh):
    shape = mesh.shape
    fine = Mesh(
        mesh.devices.reshape(shape["ia"], shape["ja"] // 2, 2, shape["ka"]), (IA, JX, JZ, KA)
    )
    placed = (
        P(IA, (JX, JZ), KA, None, None),
        P(IA, (JX, JZ), KA),
        P(IA, (JX, JZ), KA, None, None, None),
        P((IA, JX, JZ, KA), None),
        P((JX, JZ, KA), None),
        P(KA, IA),
    )
    return jax.shard_map(
        local, mesh=fine, in_specs=placed, out_specs=P((IA, JX, JZ, KA), None), check_vma=False
    )
```

```python
import jax
import jax.numpy as jnp
from jax import lax
from jax.experimental import pallas as pl
from jax.experimental.pallas import tpu as pltpu
from jax.sharding import Mesh, PartitionSpec as P


R = 256
BS = 64
RB1 = 4
SLOTS = 4
SPAN = 1024
F32 = jnp.float32
F16 = jnp.float16
PHI_SCALE = 0.25
MASS_SCALE = 1.0 / 32.0
BF16 = jnp.bfloat16

IA = "ia"
JX = "jx"
JZ = "jz"
KA = "ka"
JK = (JX, JZ, KA)
ZK = (JZ, KA)


def swap(x, axis):
    return lax.all_to_all(x, axis, split_axis=0, concat_axis=0, tiled=True)


def from_everyone(x, axis):
    return swap(jnp.broadcast_to(x, (lax.axis_size(axis), *x.shape)), axis)


def aligned(start, size):
    return pl.ds(pl.multiple_of(start * size, size), size)


def whole():
    return pl.BlockSpec(memory_space=pltpu.VMEM)


def scalars():
    return pl.BlockSpec(memory_space=pltpu.SMEM)


def load_kernel(live, counts, hits, raw, arrived):
    def fetch(slot):
        return pltpu.make_async_copy(counts.at[slot], raw.at[slot], arrived.at[slot])

    for slot in range(SLOTS):

        @pl.when(slot < live[0])
        def _():
            fetch(slot).start()

    def step(slot, carry):
        fetch(slot).wait()
        hits[slot] = raw[slot].astype(F32).astype(BF16)
        return carry

    lax.fori_loop(0, live[0], step, 0)


def load(live, counts):
    return pl.pallas_call(
        load_kernel,
        in_specs=[scalars(), pl.BlockSpec(memory_space=pltpu.HBM)],
        out_specs=whole(),
        out_shape=jax.ShapeDtypeStruct((SLOTS, BS, BS * BS), BF16),
        scratch_shapes=[
            pltpu.VMEM((SLOTS, BS, BS * BS), jnp.int32),
            pltpu.SemaphoreType.DMA((SLOTS,)),
        ],
        compiler_params=pltpu.CompilerParams(vmem_limit_bytes=10 << 20),
        name="load",
    )(live, pltpu.with_memory_space_constraint(counts, pltpu.HBM))


def prep_kernel(coords, live, both, rows_c, mass):
    rows_c[...] = jnp.swapaxes(both[:, 32:, :].reshape(R, R), 0, 1)
    mass[...] = jnp.zeros_like(mass)
    for slot in range(SLOTS):

        @pl.when(slot < live[0])
        def _():
            g = coords[slot * 3]
            j = coords[slot * 3 + 1]
            k = coords[slot * 3 + 2]
            piece_b = both[:, aligned(j, 8), :].reshape(BS, R)
            piece_c = rows_c[aligned(k, BS), :]
            sum_b = jnp.sum(piece_b, axis=0, keepdims=True)
            sum_c = jnp.sum(piece_c, axis=0, keepdims=True)
            mass[g, 0:1, :] = mass[g, 0:1, :] + sum_b * sum_c


def prepare(coords, live, both):
    return pl.pallas_call(
        prep_kernel,
        in_specs=[scalars(), scalars(), whole()],
        out_specs=[whole(), whole()],
        out_shape=[
            jax.ShapeDtypeStruct((R, R), F32),
            jax.ShapeDtypeStruct((RB1, 8, R), F32),
        ],
        compiler_params=pltpu.CompilerParams(vmem_limit_bytes=8 << 20),
        name="prepare",
    )(coords, live, both)


def pass_kernel(coords, live, hits, factor, both, rows_c, out, *panels):
    out[...] = jnp.zeros_like(out)

    def build(slot, panel):
        j = coords[slot * 3 + 1]
        piece_c = rows_c[aligned(coords[slot * 3 + 2], BS), :]
        for half in range(2):
            for sender in range(8):
                rows_b = both[sender, aligned(j, 8), :]
                for q in range(4):
                    at = ((half * 8 + sender) * 4 + q) * BS
                    row = rows_b[half * 4 + q : half * 4 + q + 1, :]
                    panel[at : at + BS, :] = (row * piece_c).astype(BF16)

    def together(first, many):
        rows = [factor[aligned(coords[(first + u) * 3], BS), :] for u in range(many)]
        total = [jnp.zeros((BS, R), F32)] * many
        for u in range(many):
            build(first + u, panels[u])
        for start in range(0, BS * BS, SPAN):
            for u in range(many):
                piece = panels[u][start : start + SPAN, :]
                model = lax.dot_general(
                    rows[u], piece, (((1,), (1,)), ((), ())), preferred_element_type=F32
                )
                count = hits[first + u, :, start : start + SPAN].astype(F32)
                ratio = (count / model).astype(BF16)
                total[u] = total[u] + jnp.dot(ratio, piece, preferred_element_type=F32)
        for u in range(many):
            i = coords[(first + u) * 3]
            out[i] = out[i] + total[u] * (rows[u].astype(F32) * PHI_SCALE)

    @pl.when(live[0] == SLOTS)
    def _():
        together(0, SLOTS)

    @pl.when(live[0] < SLOTS)
    def _():
        def step(slot, carry):
            together(slot, 1)
            return carry

        lax.fori_loop(0, live[0], step, 0)


def run_pass(coords, live, hits, factor, both, rows_c):
    return pl.pallas_call(
        pass_kernel,
        in_specs=[scalars(), scalars()] + [whole()] * 4,
        out_specs=whole(),
        scratch_shapes=[pltpu.VMEM((BS * BS, R), BF16)] * SLOTS,
        out_shape=jax.ShapeDtypeStruct((RB1, BS, R), F32),
        compiler_params=pltpu.CompilerParams(vmem_limit_bytes=24 << 20),
        name="one_pass",
    )(coords, live, hits, factor, both, rows_c)


def rounded(x):
    return lax.reduce_precision(x, exponent_bits=8, mantissa_bits=7)


def unweighted(factor, low):
    return jnp.where(low == 0.0, 0.0, factor / jnp.where(low == 0.0, 1.0, low))


def local(block_coords, live_blocks, counts, factor_a, factor_b, factor_c):
    coords = block_coords.reshape(SLOTS * 3)
    live = live_blocks.reshape(1)
    low_a = rounded(factor_a)
    mine_b = lax.dynamic_slice_in_dim(factor_b, lax.axis_index(IA) * 4, 4, 0)
    column = from_everyone(jnp.concatenate([low_a.astype(F16), mine_b.astype(F16)], axis=0), ZK)
    hits = load(live, counts.reshape(SLOTS, BS, BS * BS))
    share_b = lax.dynamic_slice_in_dim(column[:, 4:], lax.axis_index(JZ) * 8, 8, 0)
    both = from_everyone(
        jnp.concatenate([share_b.reshape(32, R), factor_c.T.astype(F16)], axis=0), IA
    ).astype(F32)
    own = column[:, :4].reshape(BS, R).astype(BF16)
    low = lax.all_gather(own, JX, axis=0, tiled=True)
    rows_c, mass = prepare(coords, live, both)

    phi = run_pass(coords, live, hits, low, both, rows_c)
    mass_rows = jnp.broadcast_to(
        (mass[:, 0, :] * MASS_SCALE).astype(F16).reshape(RB1, 1, 2, 128), (RB1, 16, 2, 128)
    ).reshape(64, 2, 128)
    sent = jnp.concatenate([phi.astype(F16).reshape(64, 2, 512), mass_rows], axis=2)
    got = swap(sent, JK).astype(F32).sum(axis=0)
    scale = (MASS_SCALE / PHI_SCALE) / got[:, 512:].reshape(1, R)
    first = unweighted(factor_a, low_a) * got[:, :512].reshape(4, R) * scale
    low_first = rounded(first)
    low = from_everyone(low_first.astype(BF16), JK).reshape(R, R)
    phi = run_pass(coords, live, hits, low, both, rows_c)
    mine = swap(phi.astype(F16).reshape(64, 4, R), JK).astype(F32).sum(axis=0)
    return unweighted(first, low_first) * mine * scale


def solution(mesh):
    shape = mesh.shape
    fine = Mesh(
        mesh.devices.reshape(shape["ia"], shape["ja"] // 2, 2, shape["ka"]), (IA, JX, JZ, KA)
    )
    placed = (
        P(IA, (JX, JZ), KA, None, None),
        P(IA, (JX, JZ), KA),
        P(IA, (JX, JZ), KA, None, None, None),
        P((IA, JX, JZ, KA), None),
        P((JX, JZ, KA), None),
        P(KA, IA),
    )
    return jax.shard_map(
        local, mesh=fine, in_specs=placed, out_specs=P((IA, JX, JZ, KA), None), check_vma=False
    )
```

```python
import functools

import jax
import jax.numpy as jnp
from jax import lax
from jax.experimental import pallas as pl
from jax.experimental.pallas import tpu as pltpu
from jax.sharding import Mesh, PartitionSpec as P


R = 256
BS = 64
RB1 = 4
SLOTS = 4
SPAN = 1024
F32 = jnp.float32
F16 = jnp.float16
PHI_SCALE = 0.25
MASS_SCALE = 1.0 / 32.0
BF16 = jnp.bfloat16

IA = "ia"
JX = "jx"
JZ = "jz"
KA = "ka"
ALL = (JZ, JX, KA)
HALF = BS // 2
ZK = (JZ, KA)


def swap(x, axis):
    return lax.all_to_all(x, axis, split_axis=0, concat_axis=0, tiled=True)


def from_everyone(x, axis):
    return swap(jnp.broadcast_to(x, (lax.axis_size(axis), *x.shape)), axis)


def aligned(start, size):
    return pl.ds(pl.multiple_of(start * size, size), size)


def whole():
    return pl.BlockSpec(memory_space=pltpu.VMEM)


def scalars():
    return pl.BlockSpec(memory_space=pltpu.SMEM)


def load_kernel(live, counts, hits, raw, arrived):
    def fetch(slot):
        return pltpu.make_async_copy(counts.at[slot], raw.at[slot], arrived.at[slot])

    for slot in range(SLOTS):

        @pl.when(slot < live[0])
        def _():
            fetch(slot).start()

    def step(slot, carry):
        fetch(slot).wait()
        hits[slot] = raw[slot].astype(F32).astype(BF16)
        return carry

    lax.fori_loop(0, live[0], step, 0)


def load(live, counts):
    return pl.pallas_call(
        load_kernel,
        in_specs=[scalars(), pl.BlockSpec(memory_space=pltpu.HBM)],
        out_specs=whole(),
        out_shape=jax.ShapeDtypeStruct((SLOTS, BS, BS * BS), BF16),
        scratch_shapes=[
            pltpu.VMEM((SLOTS, BS, BS * BS), jnp.int32),
            pltpu.SemaphoreType.DMA((SLOTS,)),
        ],
        compiler_params=pltpu.CompilerParams(vmem_limit_bytes=10 << 20),
        name="load",
    )(live, pltpu.with_memory_space_constraint(counts, pltpu.HBM))


def prep_kernel(coords, live, both, rows_c, mass):
    rows_c[...] = jnp.swapaxes(both[:, 32:, :].reshape(R, R), 0, 1)
    mass[...] = jnp.zeros_like(mass)
    for slot in range(SLOTS):

        @pl.when(slot < live[0])
        def _():
            g = coords[slot * 3]
            j = coords[slot * 3 + 1]
            k = coords[slot * 3 + 2]
            piece_b = both[:, aligned(j, 8), :].reshape(BS, R)
            piece_c = rows_c[aligned(k, BS), :]
            sum_b = jnp.sum(piece_b, axis=0, keepdims=True)
            sum_c = jnp.sum(piece_c, axis=0, keepdims=True)
            mass[g, 0:1, :] = mass[g, 0:1, :] + sum_b * sum_c


def prepare(coords, live, both):
    return pl.pallas_call(
        prep_kernel,
        in_specs=[scalars(), scalars(), whole()],
        out_specs=[whole(), whole()],
        out_shape=[
            jax.ShapeDtypeStruct((R, R), F32),
            jax.ShapeDtypeStruct((RB1, 8, R), F32),
        ],
        compiler_params=pltpu.CompilerParams(vmem_limit_bytes=8 << 20),
        name="prepare",
    )(coords, live, both)


def pass_kernel(halves, coords, live, hits, factor, both, rows_c, out, *panels):
    out[...] = jnp.zeros_like(out)

    def build(slot, panel):
        j = coords[slot * 3 + 1]
        piece_c = rows_c[aligned(coords[slot * 3 + 2], BS), :]
        for half in range(2):
            for sender in range(8):
                rows_b = both[sender, aligned(j, 8), :]
                for q in range(4):
                    at = ((half * 8 + sender) * 4 + q) * BS
                    row = rows_b[half * 4 + q : half * 4 + q + 1, :]
                    panel[at : at + BS, :] = (row * piece_c).astype(BF16)

    def factor_rows(i):
        if not halves:
            return factor[aligned(i, BS), :]
        return jnp.concatenate(
            [factor[aligned(i + RB1 * jz, HALF), :] for jz in range(2)], axis=0
        )

    def together(first, many):
        rows = [factor_rows(coords[(first + u) * 3]) for u in range(many)]
        total = [jnp.zeros((BS, R), F32)] * many
        for u in range(many):
            build(first + u, panels[u])
        for start in range(0, BS * BS, SPAN):
            for u in range(many):
                piece = panels[u][start : start + SPAN, :]
                model = lax.dot_general(
                    rows[u], piece, (((1,), (1,)), ((), ())), preferred_element_type=F32
                )
                count = hits[first + u, :, start : start + SPAN].astype(F32)
                ratio = (count / model).astype(BF16)
                total[u] = total[u] + jnp.dot(ratio, piece, preferred_element_type=F32)
        for u in range(many):
            i = coords[(first + u) * 3]
            part = total[u] * (rows[u].astype(F32) * PHI_SCALE)
            out[0, i] = out[0, i] + part[:HALF]
            out[1, i] = out[1, i] + part[HALF:]

    @pl.when(live[0] == SLOTS)
    def _():
        together(0, SLOTS)

    @pl.when(live[0] < SLOTS)
    def _():
        def step(slot, carry):
            together(slot, 1)
            return carry

        lax.fori_loop(0, live[0], step, 0)


def run_pass(halves, coords, live, hits, factor, both, rows_c):
    return pl.pallas_call(
        functools.partial(pass_kernel, halves),
        in_specs=[scalars(), scalars()] + [whole()] * 4,
        out_specs=whole(),
        scratch_shapes=[pltpu.VMEM((BS * BS, R), BF16)] * SLOTS,
        out_shape=jax.ShapeDtypeStruct((2, RB1, HALF, R), F32),
        compiler_params=pltpu.CompilerParams(vmem_limit_bytes=24 << 20),
        name="one_pass",
    )(coords, live, hits, factor, both, rows_c)


def rounded(x):
    return lax.reduce_precision(x, exponent_bits=8, mantissa_bits=7)


def unweighted(factor, low):
    return jnp.where(low == 0.0, 0.0, factor / jnp.where(low == 0.0, 1.0, low))


def local(block_coords, live_blocks, counts, factor_a, factor_b, factor_c):
    coords = block_coords.reshape(SLOTS * 3)
    live = live_blocks.reshape(1)
    low_a = rounded(factor_a)
    mine_b = lax.dynamic_slice_in_dim(factor_b, lax.axis_index(IA) * 4, 4, 0)
    column = from_everyone(
        jnp.concatenate([low_a.astype(F16), mine_b.astype(F16)], axis=0), ZK
    )
    hits = load(live, counts.reshape(SLOTS, BS, BS * BS))
    share_b = lax.dynamic_slice_in_dim(column[:, 4:], lax.axis_index(JZ) * 8, 8, 0)
    both = from_everyone(
        jnp.concatenate([share_b.reshape(32, R), factor_c.T.astype(F16)], axis=0), IA
    ).astype(F32)
    own = column[:, :4].reshape(BS, R).astype(BF16)
    low = lax.all_gather(own, JX, axis=0, tiled=True)
    rows_c, mass = prepare(coords, live, both)

    phi = run_pass(False, coords, live, hits, low, both, rows_c)
    mass_rows = jnp.broadcast_to(
        (mass[:, 0, :] * MASS_SCALE).astype(F16).reshape(1, RB1, 1, 2, 128),
        (2, RB1, 8, 2, 128),
    ).reshape(64, 2, 128)
    sent = jnp.concatenate([phi.astype(F16).reshape(64, 2, 512), mass_rows], axis=2)
    got = swap(sent, ALL).astype(F32).sum(axis=0)
    scale = (MASS_SCALE / PHI_SCALE) / got[:, 512:].reshape(1, R)
    first = unweighted(factor_a, low_a) * got[:, :512].reshape(4, R) * scale
    low_first = rounded(first)
    low = from_everyone(low_first.astype(BF16), ALL).reshape(R, R)
    phi = run_pass(True, coords, live, hits, low, both, rows_c)
    mine = swap(phi.astype(F16).reshape(64, 4, R), ALL).astype(F32).sum(axis=0)
    return unweighted(first, low_first) * mine * scale


def solution(mesh):
    shape = mesh.shape
    fine = Mesh(
        mesh.devices.reshape(shape["ia"], shape["ja"] // 2, 2, shape["ka"]), (IA, JX, JZ, KA)
    )
    placed = (
        P(IA, (JX, JZ), KA, None, None),
        P(IA, (JX, JZ), KA),
        P(IA, (JX, JZ), KA, None, None, None),
        P((IA, JX, JZ, KA), None),
        P((JX, JZ, KA), None),
        P(KA, IA),
    )
    return jax.shard_map(
        local, mesh=fine, in_specs=placed, out_specs=P((IA, JX, JZ, KA), None), check_vma=False
    )
```

```python
import functools

import jax
import jax.numpy as jnp
from jax import lax
from jax.experimental import pallas as pl
from jax.experimental.pallas import tpu as pltpu
from jax.sharding import Mesh, PartitionSpec as P


R = 256
BS = 64
RB1 = 4
SLOTS = 4
SPAN = 1024
F32 = jnp.float32
F16 = jnp.float16
PHI_SCALE = 0.25
MASS_SCALE = 1.0 / 32.0
BF16 = jnp.bfloat16


IA = "ia"
JX = "jx"
JZ = "jz"
KA = "ka"
JK = (JX, JZ, KA)
ZK = (JZ, KA)


def swap(x, axis):
    return lax.all_to_all(x, axis, split_axis=0, concat_axis=0, tiled=True)


def from_everyone(x, axis):
    return swap(jnp.broadcast_to(x, (lax.axis_size(axis), *x.shape)), axis)


def aligned(start, size):
    return pl.ds(pl.multiple_of(start * size, size), size)


def whole():
    return pl.BlockSpec(memory_space=pltpu.VMEM)


def scalars():
    return pl.BlockSpec(memory_space=pltpu.SMEM)


def load_kernel(live, counts, hits, raw, arrived):
    def fetch(slot):
        return pltpu.make_async_copy(counts.at[slot], raw.at[slot], arrived.at[slot])

    for slot in range(SLOTS):

        @pl.when(slot < live[0])
        def _():
            fetch(slot).start()

    def step(slot, carry):
        fetch(slot).wait()
        hits[slot] = raw[slot].astype(F32).astype(BF16)
        return carry

    lax.fori_loop(0, live[0], step, 0)


def load(live, counts):
    return pl.pallas_call(
        load_kernel,
        in_specs=[scalars(), pl.BlockSpec(memory_space=pltpu.HBM)],
        out_specs=whole(),
        out_shape=jax.ShapeDtypeStruct((SLOTS, BS, BS * BS), BF16),
        scratch_shapes=[
            pltpu.VMEM((SLOTS, BS, BS * BS), jnp.int32),
            pltpu.SemaphoreType.DMA((SLOTS,)),
        ],
        compiler_params=pltpu.CompilerParams(vmem_limit_bytes=10 << 20),
        name="load",
    )(live, pltpu.with_memory_space_constraint(counts, pltpu.HBM))


def prep_kernel(coords, live, both, rows_c, mass):
    rows_c[...] = jnp.swapaxes(both[:, 32:, :].reshape(R, R), 0, 1)
    mass[...] = jnp.zeros_like(mass)
    for slot in range(SLOTS):

        @pl.when(slot < live[0])
        def _():
            g = coords[slot * 3]
            j = coords[slot * 3 + 1]
            k = coords[slot * 3 + 2]
            piece_b = both[:, aligned(j, 8), :].reshape(BS, R)
            piece_c = rows_c[aligned(k, BS), :]
            sum_b = jnp.sum(piece_b, axis=0, keepdims=True)
            sum_c = jnp.sum(piece_c, axis=0, keepdims=True)
            mass[g, 0:1, :] = mass[g, 0:1, :] + sum_b * sum_c


def prepare(coords, live, both):
    return pl.pallas_call(
        prep_kernel,
        in_specs=[scalars(), scalars(), whole()],
        out_specs=[whole(), whole()],
        out_shape=[
            jax.ShapeDtypeStruct((R, R), F32),
            jax.ShapeDtypeStruct((RB1, 8, R), F32),
        ],
        compiler_params=pltpu.CompilerParams(vmem_limit_bytes=8 << 20),
        name="prepare",
    )(coords, live, both)


def pass_kernel(split, coords, live, hits, both, rows_c, *rest):
    if split:
        place, *parts, out, factor = rest[: RB1 + 3]
        panels = rest[RB1 + 3 :]
        for back in range(RB1):
            factor[back * BS : (back + 1) * BS, :] = parts[back][...]
    else:
        factor, out, *panels = rest
    out[...] = jnp.zeros_like(out)

    def build(slot, panel):
        j = coords[slot * 3 + 1]
        piece_c = rows_c[aligned(coords[slot * 3 + 2], BS), :]
        for half in range(2):
            for sender in range(8):
                rows_b = both[sender, aligned(j, 8), :]
                for q in range(4):
                    at = ((half * 8 + sender) * 4 + q) * BS
                    row = rows_b[half * 4 + q : half * 4 + q + 1, :]
                    panel[at : at + BS, :] = (row * piece_c).astype(BF16)

    def factor_rows(i):
        at = (place[0] - i) & (RB1 - 1) if split else i
        return factor[aligned(at, BS), :]

    def together(first, many):
        rows = [factor_rows(coords[(first + u) * 3]) for u in range(many)]
        total = [jnp.zeros((BS, R), F32)] * many
        for u in range(many):
            build(first + u, panels[u])
        for start in range(0, BS * BS, SPAN):
            for u in range(many):
                piece = panels[u][start : start + SPAN, :]
                model = lax.dot_general(
                    rows[u], piece, (((1,), (1,)), ((), ())), preferred_element_type=F32
                )
                count = hits[first + u, :, start : start + SPAN].astype(F32)
                ratio = (count / model).astype(BF16)
                total[u] = total[u] + jnp.dot(ratio, piece, preferred_element_type=F32)
        for u in range(many):
            i = coords[(first + u) * 3]
            out[i] = out[i] + total[u] * (rows[u].astype(F32) * PHI_SCALE)

    @pl.when(live[0] == SLOTS)
    def _():
        together(0, SLOTS)

    @pl.when(live[0] < SLOTS)
    def _():
        def step(slot, carry):
            together(slot, 1)
            return carry

        lax.fori_loop(0, live[0], step, 0)


def run_pass(coords, live, hits, both, rows_c, place, *factor):
    split = place is not None
    extra = [place] if split else []
    scratch = [pltpu.VMEM((R, R), BF16)] if split else []
    return pl.pallas_call(
        functools.partial(pass_kernel, split),
        in_specs=[scalars(), scalars(), whole(), whole(), whole()]
        + [scalars()] * len(extra)
        + [whole()] * len(factor),
        out_specs=whole(),
        scratch_shapes=scratch + [pltpu.VMEM((BS * BS, R), BF16)] * SLOTS,
        out_shape=jax.ShapeDtypeStruct((RB1, BS, R), F32),
        compiler_params=pltpu.CompilerParams(vmem_limit_bytes=24 << 20),
        name="one_pass",
    )(coords, live, hits, both, rows_c, *extra, *factor)


def rounded(x):
    return lax.reduce_precision(x, exponent_bits=8, mantissa_bits=7)


def unweighted(factor, low):
    return jnp.where(low == 0.0, 0.0, factor / jnp.where(low == 0.0, 1.0, low))


def local(block_coords, live_blocks, counts, factor_a, factor_b, factor_c):
    coords = block_coords.reshape(SLOTS * 3)
    live = live_blocks.reshape(1)
    low_a = rounded(factor_a)
    mine_b = lax.dynamic_slice_in_dim(factor_b, lax.axis_index(IA) * 4, 4, 0)
    column = from_everyone(jnp.concatenate([low_a.astype(F16), mine_b.astype(F16)], axis=0), ZK)
    hits = load(live, counts.reshape(SLOTS, BS, BS * BS))
    share_b = lax.dynamic_slice_in_dim(column[:, 4:], lax.axis_index(JZ) * 8, 8, 0)
    both = from_everyone(
        jnp.concatenate([share_b.reshape(32, R), factor_c.T.astype(F16)], axis=0), IA
    ).astype(F32)
    own = column[:, :4].reshape(BS, R).astype(BF16)
    pieces = {0: own}
    for back in (2, 1, 3):
        pieces[back] = lax.ppermute(own, JX, [(x, (x + back) % 4) for x in range(4)])
    rows_c, mass = prepare(coords, live, both)

    place = lax.axis_index(JX).reshape(1)
    phi = run_pass(coords, live, hits, both, rows_c, place, *[pieces[d] for d in range(4)])
    mass_rows = jnp.broadcast_to(
        (mass[:, 0, :] * MASS_SCALE).astype(F16).reshape(RB1, 1, 2, 128), (RB1, 16, 2, 128)
    ).reshape(64, 2, 128)
    sent = jnp.concatenate([phi.astype(F16).reshape(64, 2, 512), mass_rows], axis=2)
    got = swap(sent, JK).astype(F32).sum(axis=0)
    scale = (MASS_SCALE / PHI_SCALE) / got[:, 512:].reshape(1, R)
    first = unweighted(factor_a, low_a) * got[:, :512].reshape(4, R) * scale
    low_first = rounded(first)
    low = from_everyone(low_first.astype(BF16), JK).reshape(R, R)
    phi = run_pass(coords, live, hits, both, rows_c, None, low)
    mine = swap(phi.astype(F16).reshape(64, 4, R), JK).astype(F32).sum(axis=0)
    return unweighted(first, low_first) * mine * scale


def solution(mesh):
    shape = mesh.shape
    fine = Mesh(
        mesh.devices.reshape(shape["ia"], shape["ja"] // 2, 2, shape["ka"]), (IA, JX, JZ, KA)
    )
    placed = (
        P(IA, (JX, JZ), KA, None, None),
        P(IA, (JX, JZ), KA),
        P(IA, (JX, JZ), KA, None, None, None),
        P((IA, JX, JZ, KA), None),
        P((JX, JZ, KA), None),
        P(KA, IA),
    )
    return jax.shard_map(
        local, mesh=fine, in_specs=placed, out_specs=P((IA, JX, JZ, KA), None), check_vma=False
    )
```
